256 devices in a mesh: row: 32 (over z, x), col: 8 (over y, core).
Axes of the slice: x: 4, y: 4, z: 8, core: 2. Of those that a mesh axis runs over, the one named last changes fastest.
Arguments:
- slab: float32 [16384, 4096], P('row', 'col'), may hold values from -32 to 32, as said below
Outputs:
- factored: float32 [16384, 4096], P('row', 'col')
The draws below stay inside these ranges and needn't reach their ends.
Inputs may be any that keep to these rules, and one draw needn't show every extreme that they name: The slab holds the first 4096 columns of a symmetric positive definite matrix of order 16384, column blocks of 256 in the stored order of the first step.
All inputs are finite; a program needn't handle non-finite values.
Results may differ from the reference program's by a relative error of at most 0.00029.
Values sent between devices are 32-bit elements; how exact they have to be, the bound alone decides.
A program may use at most 128 MiB of HBM per device.

```python
import jax
import jax.numpy as jnp
from jax import lax

SLAB_COLS = 4096
EMBED = 768
BLOCK = 256
PANELS = 2
ROWS_DEV = 512
N_ROW = 32
N_COL = 8


RIDGE_TERM = 0.5


def draw_slab(key, part):
    rows_all = ROWS_DEV * N_ROW
    samples = jax.random.normal(key, (rows_all, EMBED), jnp.float32)
    kernel = jnp.dot(samples, samples[:SLAB_COLS].T, precision=lax.Precision.HIGHEST, preferred_element_type=jnp.float32) / EMBED
    kernel = kernel + RIDGE_TERM * jnp.eye(rows_all, SLAB_COLS, dtype=jnp.float32)
    return kernel.reshape(rows_all, SLAB_COLS // (BLOCK * N_COL), N_COL, BLOCK).transpose(0, 2, 1, 3).reshape(rows_all, SLAB_COLS)


def setup_inputs(seed: int = 0) -> dict:
    keys = jax.random.split(jax.random.key(seed), 2)
    slab = draw_slab(jax.random.fold_in(keys[1], 71), 0)
    return dict(slab=slab)


PRECISE = lax.Precision.HIGHEST

def to_logical(stored):
    count = stored.shape[0]
    return stored.reshape(count, N_COL, -1, BLOCK).transpose(0, 2, 1, 3).reshape(count, -1)

def to_stored(logical):
    count = logical.shape[0]
    return logical.reshape(count, -1, N_COL, BLOCK).transpose(0, 2, 1, 3).reshape(count, -1)

def reference(slab):
    state = to_logical(slab)
    row_ids = jnp.arange(state.shape[0], dtype=jnp.int32)
    identity = jnp.eye(BLOCK, dtype=jnp.float32)
    for sub_step in range(2 * PANELS):
        start = sub_step * BLOCK
        stop = start + BLOCK
        diag_tile = state[start:stop, start:stop]
        lower_factor = jnp.linalg.cholesky(diag_tile)
        inverse = jax.scipy.linalg.solve_triangular(lower_factor, identity, lower=True)
        column = jnp.dot(state[:, start:stop].astype(jnp.float32), inverse.T.astype(jnp.float32), precision=PRECISE, preferred_element_type=jnp.float32)
        column = jnp.where(row_ids[:, None] < start, jnp.float32(0.0), column)
        column = column.at[start:stop].set(lower_factor)
        state = state.at[:, start:stop].set(column)
        if sub_step % 2 == 0:
            following = state[:, stop:stop + BLOCK] - jnp.dot(column.astype(jnp.float32), column[stop:stop + BLOCK].T.astype(jnp.float32), precision=PRECISE, preferred_element_type=jnp.float32)
            state = state.at[:, stop:stop + BLOCK].set(following)
        else:
            panel_left = state[:, start - BLOCK:stop]
            remaining = state[:, stop:]
            updated = remaining - jnp.dot(panel_left.astype(jnp.float32), panel_left[stop:SLAB_COLS].T.astype(jnp.float32), precision=PRECISE, preferred_element_type=jnp.float32)
            updated = jnp.where(row_ids[:, None] >= stop, updated, remaining)
            state = state.at[:, stop:].set(updated)
    return to_stored(state)
```

```python
import functools

import jax
import jax.numpy as jnp
from jax import lax
from jax.experimental import pallas as pl
from jax.experimental.pallas import tpu as pltpu
from jax.sharding import PartitionSpec as P

F32, BF16 = jnp.float32, jnp.bfloat16
NN = (((1,), (0,)), ((), ()))
NT = (((1,), (1,)), ((), ()))
TN = (((0,), (0,)), ((), ()))
MESH = pl.DeviceIdType.MESH
TILE = 32
HALF = 128
BLOCK = 256
SIDE = 4 * BLOCK
STRIP = 512
CUT = 64


def split2(x):
    high = x.astype(BF16)
    return high, (x - high.astype(F32)).astype(BF16)


def split3(x):
    high = x.astype(BF16)
    rest = x - high.astype(F32)
    mid = rest.astype(BF16)
    return high, mid, (rest - mid.astype(F32)).astype(BF16)


def product(left, right, dims):
    def dot(a, b):
        return lax.dot_general(a, b, dims, preferred_element_type=F32)

    return dot(left[0], right[0]) + (dot(left[0], right[1]) + dot(left[1], right[0]))


def tile_step(work, t, carry):
    n = TILE
    groups = n // 8
    a = pl.multiple_of(t * n, n)
    lane = lax.broadcasted_iota(jnp.int32, (8, HALF), 1)
    row = lax.broadcasted_iota(jnp.int32, (8, HALF), 0)
    left = [work[pl.ds(a + 8 * g, 8), 0:HALF] for g in range(groups)]
    right = [work[pl.ds(a + 8 * g, 8), HALF : 2 * HALF] for g in range(groups)]

    def spread(x, i):
        return jnp.broadcast_to(x[i : i + 1, :], (8, HALF))

    columns = {}
    for j in range(n):
        chosen = lane == a + j
        for g in range(j // 8, groups):
            only = jnp.sum(jnp.where(chosen, left[g], 0.0), axis=1, keepdims=True)
            columns[j, g] = jnp.broadcast_to(only, (8, HALF))
    scale = [jnp.zeros((8, HALF), F32) for _ in range(groups)]
    for j in range(n):
        own, at = j // 8, j % 8
        root = lax.rsqrt(spread(columns[j, own], at))
        scale[own] = jnp.where(row == at, root, scale[own])
        inverse = root * root
        factor = {}
        for g in range(own, groups):
            base = jnp.where(row > at, columns[j, g], 0.0) if g == own else columns[j, g]
            factor[g] = base * inverse
        for k in range(j + 1, n):
            other = spread(columns[j, k // 8], k % 8)
            for g in range(k // 8, groups):
                columns[k, g] = columns[k, g] - factor[g] * other
        left_row, right_row = spread(left[own], at), spread(right[own], at)
        for g in range(own, groups):
            left[g] = left[g] - factor[g] * left_row
            right[g] = right[g] - factor[g] * right_row
    for g in range(groups):
        left[g] = jnp.where(lane >= a + 8 * g + row, left[g] * scale[g], 0.0)
        right[g] = right[g] * scale[g]
    upper = jnp.concatenate(left, axis=0)
    both = jnp.concatenate([upper, jnp.concatenate(right, axis=0)], axis=1)
    below = lax.broadcasted_iota(jnp.int32, (n, HALF), 1) >= a + n
    lh, lm, ll = split3(jnp.where(below, upper, 0.0))
    bh, bm, bl = split3(both)
    lefts = jnp.concatenate([lh, lh, lm, lh, ll, lm], axis=0)
    boths = jnp.concatenate([bh, bm, bh, bl, bh, bm], axis=0)
    work[...] = work[...] - lax.dot_general(lefts, boths, TN, preferred_element_type=F32)
    work[pl.ds(a, n), :] = both
    return carry


def inverse_factor(work, tile):
    rows = lax.broadcasted_iota(jnp.int32, (HALF, HALF), 0)
    cols = lax.broadcasted_iota(jnp.int32, (HALF, HALF), 1)
    work[:, 0:HALF] = tile
    work[:, HALF : 2 * HALF] = jnp.where(rows == cols, 1.0, 0.0)
    lax.fori_loop(0, HALF // TILE, functools.partial(tile_step, work), 0)
    return work[:, HALF : 2 * HALF]


class Place:
    def __init__(self):
        self.row = lax.axis_index("row")
        self.col = lax.axis_index("col")
        self.z, self.x = self.row // 4, self.row % 4
        self.y, self.core = self.col // 2, self.col % 2

    def near(self, z=0, x=0, y=0, core=0):
        row = (self.z + z + 8) % 8 * 4 + (self.x + x + 4) % 4
        col = (self.y + y + 4) % 4 * 2 + (self.core + core) % 2
        return row, col


STEPS = dict(
    yu=dict(y=1), yd=dict(y=-1), zu=dict(z=1), zd=dict(z=-1), xu=dict(x=1), xd=dict(x=-1), core=dict(core=1)
)
ORDER = ("yu", "yd", "zu", "zd", "xu", "xd", "core")


def star(at, start, up, down):
    relay = at == 3 - start
    return (
        (at == start) | (relay & (start == 1)),
        (at == start) | (relay & (start == 0)),
    )


def relays(me, ref, sems, slot, conds):
    send, recv = sems
    found = []
    for i, name in enumerate(ORDER):
        if name in conds:
            copy = pltpu.make_async_remote_copy(
                src_ref=ref,
                dst_ref=ref,
                send_sem=send.at[slot, i],
                recv_sem=recv.at[slot],
                device_id=me.near(**STEPS[name]),
                device_id_type=MESH,
            )
            found.append((conds[name], copy))
    return found


def corner_chunk(me, corner, sems, big, m):
    c, part = m // 2, m % 2
    source_row = big // 2
    slot = big * (big + 1) + m
    rows = pl.ds(pl.multiple_of(BLOCK * big + HALF * part, HALF), HALF)
    ref = corner.at[rows, pl.ds(pl.multiple_of(BLOCK * c, BLOCK), BLOCK)]
    start_y = c // 2
    mine = me.core == c % 2
    lane = mine & (me.x == source_row)
    root = lane & (me.z == 0)
    yu, yd = star(me.y, start_y, None, None)
    xu, xd = star(me.x, source_row, None, None)
    conds = dict(
        yu=root & yu,
        yd=root & yd,
        zu=lane & (me.z <= 3),
        zd=lane & ((me.z == 0) | (me.z >= 6)),
        xu=mine & xu,
        xd=mine & xd,
        core=mine,
    )
    local_row = (BLOCK * big + HALF * part) % STRIP
    return ref, slot, conds, root & (me.y == start_y), local_row


def column_chunk(me, columns, sems, h, j):
    slot = 20 + 8 * h + j
    rows = pl.ds(pl.multiple_of(STRIP * h + CUT * j, CUT), CUT)
    ref = columns.at[rows, :]
    lane = me.x == h
    xu, xd = star(me.x, h, None, None)
    conds = dict(zu=lane & (me.z <= 3), zd=lane & ((me.z == 0) | (me.z >= 6)), xu=xu, xd=xd)
    return ref, slot, conds, lane & (me.z == 0), CUT * j


def strip_chunk(me, strip, sems, c, j):
    slot = 36 + 4 * c + j
    rows = pl.ds(pl.multiple_of(HALF * j, HALF), HALF)
    ref = strip.at[rows, pl.ds(pl.multiple_of(BLOCK * c, BLOCK), BLOCK)]
    start_y = c // 2
    mine = me.core == c % 2
    yu, yd = star(me.y, start_y, None, None)
    return ref, slot, dict(yu=mine & yu, yd=mine & yd, core=mine), mine & (me.y == start_y), HALF * j


def load(slab, sems, chunk, height, width):
    ref, slot, conds, local, at = chunk

    @pl.when(local)
    def _():
        rows = pl.ds(pl.multiple_of(at, CUT), height)
        pltpu.make_async_copy(slab.at[rows, 0:width], ref, sems[1].at[slot]).start()


def arrive(me, sems, chunk):
    ref, slot, conds, local, at = chunk
    pltpu.make_async_copy(ref, ref, sems[1].at[slot]).wait()
    for cond, copy in relays(me, ref, sems, slot, conds):
        pl.when(cond)(copy.start)


def finish(me, sems, chunk):
    ref, slot, conds, local, at = chunk
    for cond, copy in relays(me, ref, sems, slot, conds):
        pl.when(cond)(copy.wait_send)


def kernel(
    slab, tile_in, out, corner, strip, columns, work, edge, edge_low, side, side_low, down, down_low, inv, inv_low,
    send, recv,
):
    me = Place()
    sems = (send, recv)
    barrier = pltpu.get_barrier_semaphore()
    for name in ORDER:
        pl.semaphore_signal(barrier, inc=1, device_id=me.near(**STEPS[name]), device_id_type=MESH)
    pl.semaphore_wait(barrier, len(ORDER))

    def each(action):
        for big in range(4):
            lax.fori_loop(0, 2 * big + 2, lambda m, _: action(corner_chunk(me, corner, sems, big, m), HALF, BLOCK) or 0, 0)
        for c in range(4):
            lax.fori_loop(0, 4, lambda j, _: action(strip_chunk(me, strip, sems, c, j), HALF, BLOCK) or 0, 0)
        for h in range(2):
            lax.fori_loop(0, 8, lambda j, _: action(column_chunk(me, columns, sems, h, j), CUT, STRIP) or 0, 0)

    each(lambda chunk, height, width: load(slab, sems, chunk, height, width))
    each(lambda chunk, height, width: arrive(me, sems, chunk))

    def span(i):
        return slice(BLOCK * i, BLOCK * i + BLOCK)

    for big in range(4):
        here = span(big)
        before = slice(0, BLOCK * big)
        for j in range(big):
            rest = corner[here, span(j)]
            if j:
                done = slice(0, BLOCK * j)
                rest = rest - product((edge[here, done], edge_low[here, done]), (edge[span(j), done], edge_low[span(j), done]), NT)
            edge[here, span(j)], edge_low[here, span(j)] = split2(product(split2(rest), (inv[span(j)], inv_low[span(j)]), NT))
        tile = corner[here, here]
        if big:
            row_edge = (edge[here, before], edge_low[here, before])
            tile = tile - product(row_edge, row_edge, NT)
        first = inverse_factor(work, tile[0:HALF, 0:HALF])
        first_parts = split2(first)
        link = product(split2(tile[HALF:, 0:HALF]), first_parts, NT)
        link_parts = split2(link)
        second = inverse_factor(work, tile[HALF:, HALF:] - product(link_parts, link_parts, NT))
        cross = -product(split2(second), split2(product(link_parts, first_parts, NN)), NN)
        whole = jnp.concatenate(
            [
                jnp.concatenate([first, jnp.zeros((HALF, HALF), F32)], axis=1),
                jnp.concatenate([cross, second], axis=1),
            ],
            axis=0,
        )
        inv[here, :], inv_low[here, :] = split2(whole)
        inv_parts = (inv[here], inv_low[here])
        rest = strip[:, here]
        rest_cols = columns[here, :]
        if big:
            rest = rest - product((side[:, before], side_low[:, before]), row_edge, NT)
            rest_cols = rest_cols - product(row_edge, (down[before], down_low[before]), NN)
        rest = product(split2(rest), inv_parts, NT)
        side[:, here], side_low[:, here] = split2(rest)

        @pl.when(me.col == big)
        def _(big=big, rest=rest):
            rows = lax.broadcasted_iota(jnp.int32, (STRIP, BLOCK), 0) + me.row * STRIP
            cols = lax.broadcasted_iota(jnp.int32, (STRIP, BLOCK), 1) + BLOCK * big
            out[:, 0:BLOCK] = jnp.where(cols <= rows, rest, 0.0)

        down[here, :], down_low[here, :] = split2(product(inv_parts, split2(rest_cols), NN))

    result = tile_in[...]
    for panel in range(2):
        part = slice(STRIP * panel, STRIP * panel + STRIP)
        change = product((side[:, part], side_low[:, part]), (down[part], down_low[part]), NN)
        result = jnp.where(me.row > panel, result - change, result)
    out[:, BLOCK:] = result[:, BLOCK:]

    @pl.when(me.col >= 4)
    def _():
        out[:, 0:BLOCK] = result[:, 0:BLOCK]

    each(lambda chunk, height, width: finish(me, sems, chunk))


def shards(slab):
    vmem = pl.BlockSpec(memory_space=pltpu.VMEM)
    return pl.pallas_call(
        kernel,
        out_shape=jax.ShapeDtypeStruct(slab.shape, F32),
        in_specs=[pl.BlockSpec(memory_space=pl.ANY), vmem],
        out_specs=vmem,
        scratch_shapes=[
            pltpu.VMEM((SIDE, SIDE), F32),
            pltpu.VMEM((STRIP, SIDE), F32),
            pltpu.VMEM((SIDE, STRIP), F32),
            pltpu.VMEM((HALF, 2 * HALF), F32),
            pltpu.VMEM((SIDE, SIDE), BF16),
            pltpu.VMEM((SIDE, SIDE), BF16),
            pltpu.VMEM((STRIP, SIDE), BF16),
            pltpu.VMEM((STRIP, SIDE), BF16),
            pltpu.VMEM((SIDE, STRIP), BF16),
            pltpu.VMEM((SIDE, STRIP), BF16),
            pltpu.VMEM((SIDE, BLOCK), BF16),
            pltpu.VMEM((SIDE, BLOCK), BF16),
            pltpu.SemaphoreType.DMA((52, len(ORDER))),
            pltpu.SemaphoreType.DMA((52,)),
        ],
        compiler_params=pltpu.CompilerParams(collective_id=0, has_side_effects=True, vmem_limit_bytes=48 * 2**20),
    )(slab, slab)


def solution(mesh):
    spec = P("row", "col")
    return jax.shard_map(shards, mesh=mesh, in_specs=(spec,), out_specs=spec, check_vma=False)
```

```python
import functools

import jax
import jax.numpy as jnp
from jax import lax
from jax.experimental import pallas as pl
from jax.experimental.pallas import tpu as pltpu
from jax.sharding import PartitionSpec as P

F32, BF16 = jnp.float32, jnp.bfloat16
NN = (((1,), (0,)), ((), ()))
NT = (((1,), (1,)), ((), ()))
TN = (((0,), (0,)), ((), ()))
MESH = pl.DeviceIdType.MESH
TILE = 32
HALF = 128
BLOCK = 256
SIDE = 4 * BLOCK
STRIP = 512
CUT = 64


def split2(x):
    high = x.astype(BF16)
    return high, (x - high.astype(F32)).astype(BF16)


def split3(x):
    high = x.astype(BF16)
    rest = x - high.astype(F32)
    mid = rest.astype(BF16)
    return high, mid, (rest - mid.astype(F32)).astype(BF16)


def product(left, right, dims):
    def dot(a, b):
        return lax.dot_general(a, b, dims, preferred_element_type=F32)

    return dot(left[0], right[0]) + (dot(left[0], right[1]) + dot(left[1], right[0]))


def tile_step(work, t, carry):
    n = TILE
    groups = n // 8
    a = pl.multiple_of(t * n, n)
    lane = lax.broadcasted_iota(jnp.int32, (8, HALF), 1)
    row = lax.broadcasted_iota(jnp.int32, (8, HALF), 0)
    left = [work[pl.ds(a + 8 * g, 8), 0:HALF] for g in range(groups)]
    right = [work[pl.ds(a + 8 * g, 8), HALF : 2 * HALF] for g in range(groups)]

    def spread(x, i):
        return jnp.broadcast_to(x[i : i + 1, :], (8, HALF))

    columns = {}
    for j in range(n):
        chosen = lane == a + j
        for g in range(j // 8, groups):
            only = jnp.sum(jnp.where(chosen, left[g], 0.0), axis=1, keepdims=True)
            columns[j, g] = jnp.broadcast_to(only, (8, HALF))
    scale = [jnp.zeros((8, HALF), F32) for _ in range(groups)]
    for j in range(n):
        own, at = j // 8, j % 8
        root = lax.rsqrt(spread(columns[j, own], at))
        scale[own] = jnp.where(row == at, root, scale[own])
        inverse = root * root
        factor = {}
        for g in range(own, groups):
            base = jnp.where(row > at, columns[j, g], 0.0) if g == own else columns[j, g]
            factor[g] = base * inverse
        for k in range(j + 1, n):
            other = spread(columns[j, k // 8], k % 8)
            for g in range(k // 8, groups):
                columns[k, g] = columns[k, g] - factor[g] * other
        left_row, right_row = spread(left[own], at), spread(right[own], at)
        for g in range(own, groups):
            left[g] = left[g] - factor[g] * left_row
            right[g] = right[g] - factor[g] * right_row
    for g in range(groups):
        left[g] = jnp.where(lane >= a + 8 * g + row, left[g] * scale[g], 0.0)
        right[g] = right[g] * scale[g]
    upper = jnp.concatenate(left, axis=0)
    both = jnp.concatenate([upper, jnp.concatenate(right, axis=0)], axis=1)
    below = lax.broadcasted_iota(jnp.int32, (n, HALF), 1) >= a + n
    lh, lm, ll = split3(jnp.where(below, upper, 0.0))
    bh, bm, bl = split3(both)
    lefts = jnp.concatenate([lh, lh, lm, lh, ll, lm], axis=0)
    boths = jnp.concatenate([bh, bm, bh, bl, bh, bm], axis=0)
    work[...] = work[...] - lax.dot_general(lefts, boths, TN, preferred_element_type=F32)
    work[pl.ds(a, n), :] = both
    return carry


def inverse_factor(work, tile):
    rows = lax.broadcasted_iota(jnp.int32, (HALF, HALF), 0)
    cols = lax.broadcasted_iota(jnp.int32, (HALF, HALF), 1)
    work[:, 0:HALF] = tile
    work[:, HALF : 2 * HALF] = jnp.where(rows == cols, 1.0, 0.0)
    lax.fori_loop(0, HALF // TILE, functools.partial(tile_step, work), 0)
    return work[:, HALF : 2 * HALF]


class Place:
    def __init__(self):
        self.row = lax.axis_index("row")
        self.col = lax.axis_index("col")
        self.z, self.x = self.row // 4, self.row % 4
        self.y, self.core = self.col // 2, self.col % 2
        self.root = (self.row == 0) & (self.col == 0)

    def near(self, z=0, x=0, y=0, core=0):
        row = (self.z + z + 8) % 8 * 4 + (self.x + x + 4) % 4
        col = (self.y + y + 4) % 4 * 2 + (self.core + core) % 2
        return row, col


STEPS = dict(y1=dict(y=1), ym1=dict(y=-1), z1=dict(z=1), zm1=dict(z=-1), x1=dict(x=1), xm1=dict(x=-1), core=dict(core=1))
ORDER = tuple(STEPS)
STARTS = (16, 28, 36)


def star(at, start):
    gap = (at - start + 4) % 4
    rising = (start == 1) | (start == 2)
    return (gap == 0) | ((gap == 1) & rising), (gap == 0) | ((gap == 3) & (rising == False))


def relays(me, ref, sems, slot, conds):
    send, recv = sems
    for i, name in enumerate(ORDER):
        if name in conds:
            copy = pltpu.make_async_remote_copy(
                src_ref=ref,
                dst_ref=ref,
                send_sem=send.at[slot, i],
                recv_sem=recv.at[slot],
                device_id=me.near(**STEPS[name]),
                device_id_type=MESH,
            )
            yield conds[name], copy


def ends(me, lane):
    return lane & (me.z <= 3), lane & ((me.z == 0) | (me.z >= 6))


def root_chunk(me, ref, slot):
    zu, zd = ends(me, (me.x == 0) & (me.y == 0))
    xu, xd = star(me.x, 0)
    yu, yd = star(me.y, 0)
    conds = dict(z1=zu, zm1=zd, x1=(me.y == 0) & xu, xm1=(me.y == 0) & xd, y1=yu, ym1=yd, core=me.core == 0)
    return ref, slot, conds, me.root, 0


def inverse_chunk(me, invs, big, i):
    rows = pl.ds(pl.multiple_of(BLOCK * big + CUT * i, CUT), CUT)
    return root_chunk(me, invs.at[rows, :], 4 * big + i)


def lower_chunk(me, lower, big, i):
    rows = pl.ds(pl.multiple_of(BLOCK * (big + 1) + CUT * i, CUT), CUT)
    return root_chunk(me, lower.at[rows, BLOCK * big : BLOCK * big + BLOCK], STARTS[big] + i)


def column_chunk(me, columns, h, j):
    slot = 40 + 8 * h + j
    rows = pl.ds(pl.multiple_of(STRIP * h + CUT * j, CUT), CUT)
    lane = me.x == h
    xu, xd = star(me.x, h)
    zu, zd = ends(me, lane)
    return columns.at[rows, :], slot, dict(z1=zu, zm1=zd, x1=xu, xm1=xd), lane & (me.z == 0), CUT * j


def strip_chunk(me, strip, c, j):
    slot = 56 + 4 * c + j
    rows = pl.ds(pl.multiple_of(HALF * j, HALF), HALF)
    ref = strip.at[rows, pl.ds(pl.multiple_of(BLOCK * c, BLOCK), BLOCK)]
    start_y = c // 2
    yu, yd = star(me.y, start_y)
    return ref, slot, dict(core=me.core >= 0, y1=yu, ym1=yd), me.y == start_y, HALF * j


class Traffic:
    def __init__(self, me, slab, lower, invs, strip, columns, sems):
        self.me, self.slab, self.sems = me, slab, sems
        self.lower, self.invs, self.strip, self.columns = lower, invs, strip, columns
        self.h = jnp.where((me.x == 0) | (me.x == 3), 0, 1)

    def load(self, chunk, height, width):
        ref, slot, conds, local, at = chunk

        @pl.when(local)
        def _():
            rows = pl.ds(pl.multiple_of(at, CUT), height)
            pltpu.make_async_copy(self.slab.at[rows, 0:width], ref, self.sems[1].at[slot]).start()

    def wait(self, chunk, *_):
        pltpu.make_async_copy(chunk[0], chunk[0], self.sems[1].at[chunk[1]]).wait()

    def send(self, chunk):
        for cond, copy in relays(self.me, chunk[0], self.sems, chunk[1], chunk[2]):
            pl.when(cond)(copy.start)

    def arrive(self, chunk, *_):
        self.wait(chunk)
        self.send(chunk)

    def begin(self, chunk, *_):
        pl.when(chunk[3])(lambda: self.arrive(chunk))

    def follow(self, chunk, *_):
        pl.when(chunk[3] == False)(lambda: self.arrive(chunk))

    def finish(self, chunk, *_):
        for cond, copy in relays(self.me, chunk[0], self.sems, chunk[1], chunk[2]):
            pl.when(cond)(copy.wait_send)

    def spread(self, chunk):
        @pl.when(self.me.root == False)
        def _():
            self.wait(chunk)
            pl.when(self.me.core == 0)(lambda: self.send(chunk))

    def inverse_spread(self, action, big, start=0, count=4):
        loop(count, lambda i: action(inverse_chunk(self.me, self.invs, big, start + i)))

    def lower_spread(self, action, big):
        if big < 3:
            loop(4 * (3 - big), lambda i: action(lower_chunk(self.me, self.lower, big, i)))

    def finish_root(self, chunk):
        pl.when(self.me.core == 0)(lambda: self.finish(chunk))

    def strip_duty(self, action, j):
        for q in range(2):
            action(strip_chunk(self.me, self.strip, self.me.core + 2 * q, j), HALF, BLOCK)

    def strip_need(self, c):
        @pl.when(self.me.core != c % 2)
        def _():
            loop(4, lambda j: self.wait(strip_chunk(self.me, self.strip, c, j)))

    def column_duty(self, action, j):
        action(column_chunk(self.me, self.columns, self.h, j), CUT, STRIP)

    def column_need(self, big):
        @pl.when(self.h != big // 2)
        def _():
            loop(4, lambda j: self.wait(column_chunk(self.me, self.columns, big // 2, 4 * (big % 2) + j)))

    def strips(self, action):
        loop(4, functools.partial(self.strip_duty, action))

    def columns_part(self, action, start, count):
        loop(count, lambda j: self.column_duty(action, start + j))


def loop(count, body):
    def one(i, carry):
        body(i)
        return carry

    lax.fori_loop(0, count, one, 0)


def blocks_to_root():
    return [(0, 1, 1)] + [(1, c, 2) for c in range(3)] + [(1, c, 3) for c in range(4)]


def span(i):
    return slice(BLOCK * i, BLOCK * i + BLOCK)


def factor_corner(traffic, corner, lower, invs, edge, edge_low, work, ready):
    for big in range(4):
        here = span(big)
        before = slice(0, BLOCK * big)
        for c in range(big + 1):
            ready(big, c)
        tile = corner[here, here]
        if big:
            row_edge = (edge[here, before], edge_low[here, before])
            tile = tile - product(row_edge, row_edge, NT)
        first = inverse_factor(work, tile[0:HALF, 0:HALF])
        first_parts = split2(first)
        top = jnp.concatenate([first, jnp.zeros((HALF, HALF), F32)], axis=1)
        invs[BLOCK * big : BLOCK * big + HALF, :] = top
        link_parts = split2(product(split2(tile[HALF:, 0:HALF]), first_parts, NT))
        traffic.inverse_spread(traffic.send, big, 0, 2)
        second = inverse_factor(work, tile[HALF:, HALF:] - product(link_parts, link_parts, NT))
        cross = -product(split2(second), split2(product(link_parts, first_parts, NN)), NN)
        bottom = jnp.concatenate([cross, second], axis=1)
        invs[BLOCK * big + HALF : BLOCK * big + BLOCK, :] = bottom
        traffic.inverse_spread(traffic.send, big, 2, 2)
        whole = jnp.concatenate([top, bottom], axis=0)
        inv_parts = split2(whole)
        for low in range(big + 1, 4):
            ready(low, big)
            rest = corner[span(low), here]
            if big:
                rest = rest - product((edge[span(low), before], edge_low[span(low), before]), row_edge, NT)
            rest = product(split2(rest), inv_parts, NT)
            lower[span(low), here] = rest
            edge[span(low), here], edge_low[span(low), here] = split2(rest)
        traffic.lower_spread(traffic.send, big)


def kernel(
    slab, out, tile_in, corner, lower, invs, strip, columns, work, edge, edge_low, side, side_low, down, down_low,
    send, recv, gather_send, gather_recv, own_sem,
):
    me = Place()
    traffic = Traffic(me, slab, lower, invs, strip, columns, (send, recv))

    @pl.when(me.root)
    def _():
        pltpu.make_async_copy(slab.at[:, 0:BLOCK], corner.at[0:STRIP, 0:BLOCK], gather_recv.at[0]).start()

    traffic.strips(traffic.load)
    traffic.columns_part(traffic.load, 0, 8)
    own = pltpu.make_async_copy(slab, tile_in, own_sem)
    own.start()
    barrier = pltpu.get_barrier_semaphore()
    for name in ORDER:
        pl.semaphore_signal(barrier, inc=1, device_id=me.near(**STEPS[name]), device_id_type=MESH)
    diagonal = (me.row == 1) & (me.col >= 1) & (me.col < 4)

    @pl.when(me.root)
    def _():
        for c in range(1, 4):
            pl.semaphore_signal(barrier, inc=1, device_id=(1, c), device_id_type=MESH)

    @pl.when(diagonal)
    def _():
        pl.semaphore_signal(barrier, inc=1, device_id=(0, 0), device_id_type=MESH)

    pl.semaphore_wait(barrier, len(ORDER) + jnp.where(me.root, 3, jnp.where(diagonal, 1, 0)))

    def to_root(row, c, big):
        at = BLOCK * big - STRIP * row
        slot = 1 + blocks_to_root().index((row, c, big))
        copy = pltpu.make_async_remote_copy(
            src_ref=slab.at[at : at + BLOCK, 0:BLOCK],
            dst_ref=corner.at[span(big), span(c)],
            send_sem=gather_send.at[slot],
            recv_sem=gather_recv.at[slot],
            device_id=(0, 0),
            device_id_type=MESH,
        )
        return (me.row == row) & (me.col == c), copy

    for block in blocks_to_root():
        sender, copy = to_root(*block)
        pl.when(sender)(copy.start)
    traffic.strips(traffic.begin)
    traffic.columns_part(traffic.begin, 0, 8)

    seen = set()

    def ready(big, c):
        if (big, c) in seen:
            return
        seen.add((big, c))
        if (big, c) == (0, 0):
            pltpu.make_async_copy(slab.at[:, 0:BLOCK], corner.at[0:STRIP, 0:BLOCK], gather_recv.at[0]).wait()
        elif (big, c) != (1, 0):
            to_root(big // 2, c, big)[1].wait_recv()

    @pl.when(me.root)
    def _():
        factor_corner(traffic, corner, lower, invs, edge, edge_low, work, ready)

    traffic.strips(traffic.follow)
    traffic.columns_part(traffic.follow, 0, 4)
    for big in range(4):
        here = span(big)
        before = slice(0, BLOCK * big)
        if big:
            traffic.strip_need(big)
            traffic.column_need(big)
        if big:
            rest = strip[:, here]
            rest_cols = columns[here, :]
            row_edge = split2(lower[here, before])
            rest = rest - product((side[:, before], side_low[:, before]), row_edge, NT)
            rest_cols = rest_cols - product(row_edge, (down[before], down_low[before]), NN)
        traffic.inverse_spread(traffic.spread, big)
        if not big:
            traffic.columns_part(traffic.follow, 4, 2)
            traffic.lower_spread(traffic.spread, 0)
            traffic.columns_part(traffic.follow, 6, 2)
            traffic.strip_need(0)
            traffic.column_need(0)
            own.wait()
            rest = strip[:, here]
            rest_cols = columns[here, :]
        inv_parts = split2(invs[here, :])
        rest = product(split2(rest), inv_parts, NT)
        side[:, here], side_low[:, here] = split2(rest)

        @pl.when(me.col == big)
        def _(big=big, rest=rest):
            rows = lax.broadcasted_iota(jnp.int32, (STRIP, BLOCK), 0) + me.row * STRIP
            cols = lax.broadcasted_iota(jnp.int32, (STRIP, BLOCK), 1) + BLOCK * big
            out[:, 0:BLOCK] = jnp.where(cols <= rows, rest, 0.0)

        down[here, :], down_low[here, :] = split2(product(inv_parts, split2(rest_cols), NN))
        if big:
            traffic.lower_spread(traffic.spread, big)
        change = product((side[:, here], side_low[:, here]), (down[here], down_low[here]), NN)
        tile_in[...] = jnp.where(me.row > big // 2, tile_in[...] - change, tile_in[...])

    result = tile_in
    out[:, BLOCK:] = result[:, BLOCK:]

    @pl.when(me.col >= 4)
    def _():
        out[:, 0:BLOCK] = result[:, 0:BLOCK]

    for big in range(4):
        traffic.inverse_spread(traffic.finish_root, big)
        traffic.lower_spread(traffic.finish_root, big)
    traffic.strips(traffic.finish)
    traffic.columns_part(traffic.finish, 0, 8)
    for block in blocks_to_root():
        sender, copy = to_root(*block)
        pl.when(sender)(copy.wait_send)


def shards(slab):
    vmem = pl.BlockSpec(memory_space=pltpu.VMEM)
    return pl.pallas_call(
        kernel,
        out_shape=jax.ShapeDtypeStruct(slab.shape, F32),
        in_specs=[pl.BlockSpec(memory_space=pl.ANY)],
        out_specs=vmem,
        scratch_shapes=[
            pltpu.VMEM((STRIP, STRIP), F32),
            pltpu.VMEM((SIDE, SIDE), F32),
            pltpu.VMEM((SIDE, SIDE), F32),
            pltpu.VMEM((SIDE, BLOCK), F32),
            pltpu.VMEM((STRIP, SIDE), F32),
            pltpu.VMEM((SIDE, STRIP), F32),
            pltpu.VMEM((HALF, 2 * HALF), F32),
            pltpu.VMEM((SIDE, SIDE), BF16),
            pltpu.VMEM((SIDE, SIDE), BF16),
            pltpu.VMEM((STRIP, SIDE), BF16),
            pltpu.VMEM((STRIP, SIDE), BF16),
            pltpu.VMEM((SIDE, STRIP), BF16),
            pltpu.VMEM((SIDE, STRIP), BF16),
            pltpu.SemaphoreType.DMA((72, len(ORDER))),
            pltpu.SemaphoreType.DMA((72,)),
            pltpu.SemaphoreType.DMA((9,)),
            pltpu.SemaphoreType.DMA((9,)),
            pltpu.SemaphoreType.DMA,
        ],
        compiler_params=pltpu.CompilerParams(collective_id=0, has_side_effects=True, vmem_limit_bytes=48 * 2**20),
    )(slab)


def solution(mesh):
    spec = P("row", "col")
    return jax.shard_map(shards, mesh=mesh, in_specs=(spec,), out_specs=spec, check_vma=False)
```

```python
import functools

import jax
import jax.numpy as jnp
from jax import lax
from jax.experimental import pallas as pl
from jax.experimental.pallas import tpu as pltpu
from jax.sharding import PartitionSpec as P

F32, BF16 = jnp.float32, jnp.bfloat16
NN = (((1,), (0,)), ((), ()))
NT = (((1,), (1,)), ((), ()))
TN = (((0,), (0,)), ((), ()))
MESH = pl.DeviceIdType.MESH
TILE = 32
HALF = 128
BLOCK = 256
SIDE = 4 * BLOCK
STRIP = 512
CUT = 64
SLICE = 32
PER_HALF = STRIP // SLICE


def split2(x):
    high = x.astype(BF16)
    return high, (x - high.astype(F32)).astype(BF16)


def split3(x):
    high = x.astype(BF16)
    rest = x - high.astype(F32)
    mid = rest.astype(BF16)
    return high, mid, (rest - mid.astype(F32)).astype(BF16)


def product(left, right, dims):
    def dot(a, b):
        return lax.dot_general(a, b, dims, preferred_element_type=F32)

    return dot(left[0], right[0]) + (dot(left[0], right[1]) + dot(left[1], right[0]))


def tile_step(work, t, carry):
    n = TILE
    groups = n // 8
    a = pl.multiple_of(t * n, n)
    lane = lax.broadcasted_iota(jnp.int32, (8, HALF), 1)
    row = lax.broadcasted_iota(jnp.int32, (8, HALF), 0)
    left = [work[pl.ds(a + 8 * g, 8), 0:HALF] for g in range(groups)]
    right = [work[pl.ds(a + 8 * g, 8), HALF : 2 * HALF] for g in range(groups)]

    def spread(x, i):
        return jnp.broadcast_to(x[i : i + 1, :], (8, HALF))

    columns = {}
    for j in range(n):
        chosen = lane == a + j
        for g in range(j // 8, groups):
            only = jnp.sum(jnp.where(chosen, left[g], 0.0), axis=1, keepdims=True)
            columns[j, g] = jnp.broadcast_to(only, (8, HALF))
    scale = [jnp.zeros((8, HALF), F32) for _ in range(groups)]
    for j in range(n):
        own, at = j // 8, j % 8
        root = lax.rsqrt(spread(columns[j, own], at))
        scale[own] = jnp.where(row == at, root, scale[own])
        inverse = root * root
        factor = {}
        for g in range(own, groups):
            base = jnp.where(row > at, columns[j, g], 0.0) if g == own else columns[j, g]
            factor[g] = base * inverse
        for k in range(j + 1, n):
            other = spread(columns[j, k // 8], k % 8)
            for g in range(k // 8, groups):
                columns[k, g] = columns[k, g] - factor[g] * other
        left_row, right_row = spread(left[own], at), spread(right[own], at)
        for g in range(own, groups):
            left[g] = left[g] - factor[g] * left_row
            right[g] = right[g] - factor[g] * right_row
    for g in range(groups):
        left[g] = jnp.where(lane >= a + 8 * g + row, left[g] * scale[g], 0.0)
        right[g] = right[g] * scale[g]
    upper = jnp.concatenate(left, axis=0)
    both = jnp.concatenate([upper, jnp.concatenate(right, axis=0)], axis=1)
    below = lax.broadcasted_iota(jnp.int32, (n, HALF), 1) >= a + n
    lh, lm, ll = split3(jnp.where(below, upper, 0.0))
    bh, bm, bl = split3(both)
    lefts = jnp.concatenate([lh, lh, lm, lh, ll, lm], axis=0)
    boths = jnp.concatenate([bh, bm, bh, bl, bh, bm], axis=0)
    work[...] = work[...] - lax.dot_general(lefts, boths, TN, preferred_element_type=F32)
    work[pl.ds(a, n), :] = both
    return carry


def inverse_factor(work, tile):
    rows = lax.broadcasted_iota(jnp.int32, (HALF, HALF), 0)
    cols = lax.broadcasted_iota(jnp.int32, (HALF, HALF), 1)
    work[:, 0:HALF] = tile
    work[:, HALF : 2 * HALF] = jnp.where(rows == cols, 1.0, 0.0)
    lax.fori_loop(0, HALF // TILE, functools.partial(tile_step, work), 0)
    return work[:, HALF : 2 * HALF]


class Place:
    def __init__(self):
        self.row = lax.axis_index("row")
        self.col = lax.axis_index("col")
        self.z, self.x = self.row // 4, self.row % 4
        self.y, self.core = self.col // 2, self.col % 2
        self.root = (self.row == 0) & (self.col == 0)
        self.peers = {name: self.near(**step) for name, step in STEPS.items()}
        self.half = jnp.where((self.x == 0) | (self.x == 3), 0, 1)
        zu, zd = ends(self, (self.x == 0) & (self.y == 0))
        xu, xd = star(self.x, 0)
        level = self.y == 0
        yu, yd = self.y <= 1, level
        self.root_conds = dict(z1=zu, zm1=zd, x1=level & xu, xm1=level & xd, y1=yu, ym1=yd, core=self.core == 0)
        xu, xd = star(self.x, self.half)
        zu, zd = ends(self, self.x == self.half)
        self.column_conds = dict(z1=zu, zm1=zd, x1=xu, xm1=xd)
        self.strip_conds = []
        for start in range(2):
            yu, yd = star(self.y, start)
            self.strip_conds.append(dict(core=self.core >= 0, y1=yu, ym1=yd))

    def near(self, z=0, x=0, y=0, core=0):
        row = (self.z + z + 8) % 8 * 4 + (self.x + x + 4) % 4
        col = (self.y + y + 4) % 4 * 2 + (self.core + core) % 2
        return row, col


STEPS = dict(y1=dict(y=1), ym1=dict(y=-1), z1=dict(z=1), zm1=dict(z=-1), x1=dict(x=1), xm1=dict(x=-1), core=dict(core=1))
ORDER = tuple(STEPS)
STARTS = (16, 22, 26)


def star(at, start):
    gap = (at - start + 4) % 4
    rising = (start == 1) | (start == 2)
    return (gap == 0) | ((gap == 1) & rising), (gap == 0) | ((gap == 3) & (rising == False))


def relays(me, ref, sems, slot, conds):
    send, recv = sems
    for i, name in enumerate(ORDER):
        if name in conds:
            copy = pltpu.make_async_remote_copy(
                src_ref=ref,
                dst_ref=ref,
                send_sem=send.at[slot, i],
                recv_sem=recv.at[slot],
                device_id=me.peers[name],
                device_id_type=MESH,
            )
            yield conds[name], copy


def ends(me, lane):
    return lane & (me.z <= 3), lane & ((me.z == 0) | (me.z >= 6))


def root_chunk(me, ref, slot):
    return ref, slot, me.root_conds, me.root, 0


def inverse_chunk(me, invs, big, i):
    rows = pl.ds(pl.multiple_of(BLOCK * big + CUT * i, CUT), CUT)
    return root_chunk(me, invs.at[rows, :], 4 * big + i)


def lower_chunk(me, lower, big, i):
    rows = pl.ds(pl.multiple_of(BLOCK * (big + 1) + HALF * i, HALF), HALF)
    return root_chunk(me, lower.at[rows, BLOCK * big : BLOCK * big + BLOCK], STARTS[big] + i)


def column_chunk(me, columns, h, j, first):
    slot = 40 + PER_HALF * h + j
    rows = pl.ds(pl.multiple_of(STRIP * h + SLICE * j, SLICE), SLICE)
    return columns.at[rows, first:STRIP], slot, me.column_conds, (me.x == h) & (me.z == 0), SLICE * j


def strip_chunk(me, strip, start, core, j):
    c = 2 * start + core
    slot = 40 + 2 * PER_HALF + 4 * c + j
    rows = pl.ds(pl.multiple_of(HALF * j, HALF), HALF)
    ref = strip.at[rows, pl.ds(pl.multiple_of(BLOCK * c, BLOCK), BLOCK)]
    return ref, slot, me.strip_conds[start], me.y == start, HALF * j


class Traffic:
    def __init__(self, me, slab, lower, invs, strip, columns, sems):
        self.me, self.slab, self.sems = me, slab, sems
        self.lower, self.invs, self.strip, self.columns = lower, invs, strip, columns
        self.h = me.half

    def load(self, chunk, height, first, last):
        ref, slot, conds, local, at = chunk

        @pl.when(local)
        def _():
            rows = pl.ds(pl.multiple_of(at, SLICE), height)
            pltpu.make_async_copy(self.slab.at[rows, first:last], ref, self.sems[1].at[slot]).start()

    def wait(self, chunk, *_):
        pltpu.make_async_copy(chunk[0], chunk[0], self.sems[1].at[chunk[1]]).wait()

    def send(self, chunk):
        for cond, copy in relays(self.me, chunk[0], self.sems, chunk[1], chunk[2]):
            pl.when(cond)(copy.start)

    def arrive(self, chunk, *_):
        self.wait(chunk)
        self.send(chunk)

    def begin(self, chunk, *_):
        pl.when(chunk[3])(lambda: self.arrive(chunk))

    def follow(self, chunk, *_):
        pl.when(chunk[3] == False)(lambda: self.arrive(chunk))

    def finish(self, chunk, *_):
        for cond, copy in relays(self.me, chunk[0], self.sems, chunk[1], chunk[2]):
            pl.when(cond)(copy.wait_send)

    def spread(self, chunk):
        @pl.when(self.me.root == False)
        def _():
            self.wait(chunk)
            pl.when(self.me.core == 0)(lambda: self.send(chunk))

    def inverse_spread(self, action, big, start=0, count=4):
        loop(count, lambda i: action(inverse_chunk(self.me, self.invs, big, start + i)))

    def lower_spread(self, action, big):
        if big < 3:
            loop(2 * (3 - big), lambda i: action(lower_chunk(self.me, self.lower, big, i)))

    def finish_root(self, chunk):
        pl.when(self.me.core == 0)(lambda: self.finish(chunk))

    def strip_duty(self, action, j):
        for q in range(2):
            action(strip_chunk(self.me, self.strip, q, self.me.core, j), HALF, 0, BLOCK)

    def strip_need(self, c):
        @pl.when(self.me.core != c % 2)
        def _():
            loop(4, lambda j: self.wait(strip_chunk(self.me, self.strip, c // 2, c % 2, j)))

    def by_width(self, body):
        pl.when(self.me.y < 2)(lambda: body(BLOCK))
        pl.when(self.me.y >= 2)(lambda: body(0))

    def column_need(self, big):
        count = BLOCK // SLICE

        def body(first):
            loop(
                count,
                lambda j: self.wait(column_chunk(self.me, self.columns, big // 2, count * (big % 2) + j, first)),
            )

        pl.when(self.h != big // 2)(lambda: self.by_width(body))

    def strips(self, action):
        loop(4, functools.partial(self.strip_duty, action))

    def columns_part(self, action, start, count):
        def body(first):
            loop(
                count,
                lambda j: action(column_chunk(self.me, self.columns, self.h, start + j, first), SLICE, first, STRIP),
            )

        self.by_width(body)


def loop(count, body):
    def one(i, carry):
        body(i)
        return carry

    lax.fori_loop(0, count, one, 0)


def blocks_to_root():
    return [(0, 1, 1)] + [(1, c, 2) for c in range(3)] + [(1, c, 3) for c in range(4)]


def span(i):
    return slice(BLOCK * i, BLOCK * i + BLOCK)


def factor_corner(traffic, corner, lower, invs, edge, edge_low, work, ready):
    for big in range(4):
        here = span(big)
        before = slice(0, BLOCK * big)
        for c in range(big + 1):
            ready(big, c)
        tile = corner[here, here]
        if big:
            row_edge = (edge[here, before], edge_low[here, before])
            tile = tile - product(row_edge, row_edge, NT)
        first = inverse_factor(work, tile[0:HALF, 0:HALF])
        first_parts = split2(first)
        top = jnp.concatenate([first, jnp.zeros((HALF, HALF), F32)], axis=1)
        invs[BLOCK * big : BLOCK * big + HALF, :] = top
        link_parts = split2(product(split2(tile[HALF:, 0:HALF]), first_parts, NT))
        traffic.inverse_spread(traffic.send, big, 0, 2)
        second = inverse_factor(work, tile[HALF:, HALF:] - product(link_parts, link_parts, NT))
        cross = -product(split2(second), split2(product(link_parts, first_parts, NN)), NN)
        bottom = jnp.concatenate([cross, second], axis=1)
        invs[BLOCK * big + HALF : BLOCK * big + BLOCK, :] = bottom
        traffic.inverse_spread(traffic.send, big, 2, 2)
        whole = jnp.concatenate([top, bottom], axis=0)
        inv_parts = split2(whole)
        for low in range(big + 1, 4):
            ready(low, big)
            rest = corner[span(low), here]
            if big:
                rest = rest - product((edge[span(low), before], edge_low[span(low), before]), row_edge, NT)
            rest = product(split2(rest), inv_parts, NT)
            lower[span(low), here] = rest
            edge[span(low), here], edge_low[span(low), here] = split2(rest)
        traffic.lower_spread(traffic.send, big)


def kernel(
    slab, out, tile_in, corner, lower, invs, strip, columns, work, edge, edge_low, side, side_low, down, down_low,
    send, recv, gather_send, gather_recv, own_sem,
):
    me = Place()
    traffic = Traffic(me, slab, lower, invs, strip, columns, (send, recv))

    @pl.when(me.root)
    def _():
        pltpu.make_async_copy(slab.at[:, 0:BLOCK], corner.at[0:STRIP, 0:BLOCK], gather_recv.at[0]).start()

    traffic.strips(traffic.load)
    traffic.columns_part(traffic.load, 0, PER_HALF)

    @pl.when(me.y < 2)
    def _():
        columns[:, 0:BLOCK] = jnp.zeros((SIDE, BLOCK), F32)

    own = pltpu.make_async_copy(slab, tile_in, own_sem)
    own.start()
    barrier = pltpu.get_barrier_semaphore()
    for name in ORDER:
        pl.semaphore_signal(barrier, inc=1, device_id=me.peers[name], device_id_type=MESH)
    diagonal = (me.row == 1) & (me.col >= 1) & (me.col < 4)

    @pl.when(me.root)
    def _():
        for c in range(1, 4):
            pl.semaphore_signal(barrier, inc=1, device_id=(1, c), device_id_type=MESH)

    @pl.when(diagonal)
    def _():
        pl.semaphore_signal(barrier, inc=1, device_id=(0, 0), device_id_type=MESH)

    pl.semaphore_wait(barrier, len(ORDER) + jnp.where(me.root, 3, jnp.where(diagonal, 1, 0)))

    def to_root(row, c, big):
        at = BLOCK * big - STRIP * row
        slot = 1 + blocks_to_root().index((row, c, big))
        copy = pltpu.make_async_remote_copy(
            src_ref=slab.at[at : at + BLOCK, 0:BLOCK],
            dst_ref=corner.at[span(big), span(c)],
            send_sem=gather_send.at[slot],
            recv_sem=gather_recv.at[slot],
            device_id=(0, 0),
            device_id_type=MESH,
        )
        return (me.row == row) & (me.col == c), copy

    for block in blocks_to_root():
        sender, copy = to_root(*block)
        pl.when(sender)(copy.start)
    traffic.strips(traffic.begin)
    traffic.columns_part(traffic.begin, 0, PER_HALF)

    seen = set()

    def ready(big, c):
        if (big, c) in seen:
            return
        seen.add((big, c))
        if (big, c) == (0, 0):
            pltpu.make_async_copy(slab.at[:, 0:BLOCK], corner.at[0:STRIP, 0:BLOCK], gather_recv.at[0]).wait()
        elif (big, c) != (1, 0):
            to_root(big // 2, c, big)[1].wait_recv()

    @pl.when(me.root)
    def _():
        factor_corner(traffic, corner, lower, invs, edge, edge_low, work, ready)

    traffic.strips(traffic.follow)
    traffic.columns_part(traffic.follow, 0, PER_HALF // 2)
    for big in range(4):
        here = span(big)
        before = slice(0, BLOCK * big)
        if big:
            traffic.strip_need(big)
            traffic.column_need(big)
        if big:
            rest = strip[:, here]
            rest_cols = columns[here, :]
            row_edge = split2(lower[here, before])
            rest = rest - product((side[:, before], side_low[:, before]), row_edge, NT)
            rest_cols = rest_cols - product(row_edge, (down[before], down_low[before]), NN)
        traffic.inverse_spread(traffic.spread, big)
        if not big:
            traffic.columns_part(traffic.follow, PER_HALF // 2, PER_HALF // 4)
            traffic.lower_spread(traffic.spread, 0)
            traffic.columns_part(traffic.follow, 3 * PER_HALF // 4, PER_HALF // 4)
            traffic.strip_need(0)
            traffic.column_need(0)
            own.wait()
            rest = strip[:, here]
            rest_cols = columns[here, :]
        inv_parts = split2(invs[here, :])
        rest = product(split2(rest), inv_parts, NT)
        side[:, here], side_low[:, here] = split2(rest)

        @pl.when(me.col == big)
        def _(big=big, rest=rest):
            rows = lax.broadcasted_iota(jnp.int32, (STRIP, BLOCK), 0) + me.row * STRIP
            cols = lax.broadcasted_iota(jnp.int32, (STRIP, BLOCK), 1) + BLOCK * big
            out[:, 0:BLOCK] = jnp.where(cols <= rows, rest, 0.0)

        down[here, :], down_low[here, :] = split2(product(inv_parts, split2(rest_cols), NN))
        if big:
            traffic.lower_spread(traffic.spread, big)
        change = product((side[:, here], side_low[:, here]), (down[here], down_low[here]), NN)
        tile_in[...] = jnp.where(me.row > big // 2, tile_in[...] - change, tile_in[...])

    result = tile_in
    out[:, BLOCK:] = result[:, BLOCK:]

    @pl.when(me.col >= 4)
    def _():
        out[:, 0:BLOCK] = result[:, 0:BLOCK]

    for big in range(4):
        traffic.inverse_spread(traffic.finish_root, big)
        traffic.lower_spread(traffic.finish_root, big)
    traffic.strips(traffic.finish)
    traffic.columns_part(traffic.finish, 0, PER_HALF)
    for block in blocks_to_root():
        sender, copy = to_root(*block)
        pl.when(sender)(copy.wait_send)


def shards(slab):
    vmem = pl.BlockSpec(memory_space=pltpu.VMEM)
    return pl.pallas_call(
        kernel,
        out_shape=jax.ShapeDtypeStruct(slab.shape, F32),
        in_specs=[pl.BlockSpec(memory_space=pl.ANY)],
        out_specs=vmem,
        scratch_shapes=[
            pltpu.VMEM((STRIP, STRIP), F32),
            pltpu.VMEM((SIDE, SIDE), F32),
            pltpu.VMEM((SIDE, SIDE), F32),
            pltpu.VMEM((SIDE, BLOCK), F32),
            pltpu.VMEM((STRIP, SIDE), F32),
            pltpu.VMEM((SIDE, STRIP), F32),
            pltpu.VMEM((HALF, 2 * HALF), F32),
            pltpu.VMEM((SIDE, SIDE), BF16),
            pltpu.VMEM((SIDE, SIDE), BF16),
            pltpu.VMEM((STRIP, SIDE), BF16),
            pltpu.VMEM((STRIP, SIDE), BF16),
            pltpu.VMEM((SIDE, STRIP), BF16),
            pltpu.VMEM((SIDE, STRIP), BF16),
            pltpu.SemaphoreType.DMA((88, len(ORDER))),
            pltpu.SemaphoreType.DMA((88,)),
            pltpu.SemaphoreType.DMA((9,)),
            pltpu.SemaphoreType.DMA((9,)),
            pltpu.SemaphoreType.DMA,
        ],
        compiler_params=pltpu.CompilerParams(collective_id=0, has_side_effects=True, vmem_limit_bytes=48 * 2**20),
    )(slab)


def solution(mesh):
    spec = P("row", "col")
    return jax.shard_map(shards, mesh=mesh, in_specs=(spec,), out_specs=spec, check_vma=False)
```
